32 devices in a mesh: grp: 2 (over y), user: 8 (over z, core), head: 2 (over x).
Axes of the slice: x: 2, y: 2, z: 4, core: 2. Of those that a mesh axis runs over, the one named last changes fastest.
Arguments:
- cand_ids: int32 [16, 512], P(('grp', 'user')), parts along dimension 0, may hold values from 0 to 4095, as said below
- prefix_len: int32 [16], P(('grp', 'user')), parts along dimension 0, may hold values from 1 to 512
- key_cache: bfloat16 [16, 512, 1024], P(('grp', 'user'), None, 'head'), parts along dimension 0, may hold values from -6 to 6
- value_cache: bfloat16 [16, 512, 1024], P(('grp', 'user'), None, 'head'), parts along dimension 0, may hold values from -6 to 6
- item_table: bfloat16 [4096, 1024], P('user'), may hold values from -6 to 6
- w_qkvu: bfloat16 [1024, 8, 4, 128], P(None, 'head'), may hold values from -0.1875 to 0.1875
- w_out: bfloat16 [8, 128, 1024], P('head'), may hold values from -0.1875 to 0.1875
Outputs:
- scores: float32 [16, 512], P(('grp', 'user')), parts along dimension 0
The draws below stay inside these ranges and needn't reach their ends.
There are 2 independent parts, one for each index of `grp`. The reference program is written for one: setup_inputs(seed, part) draws one part's arguments, and reference() takes and returns one part's arrays. A program takes and returns all parts, laid end to end along the dimension named above; an argument that names none is the same for every part. Nothing has to cross between parts.
Inputs may be any that keep to these rules, and one draw needn't show every extreme that they name: `cand_ids`: item id s * 512 + r lies in table shard s. Among the 512 candidates of each aligned block of 1 users, at most 128 lie in one table shard, and in every block some shard holds exactly 128 of them.
All inputs are finite; a program needn't handle non-finite values.
Results may differ from the reference program's by a relative error of at most 0.0095.
Values may be sent and summed in bfloat16 or wider, within the bound.
No kernel may reach another device: no remote copies, remote signals or barrier semaphores. Data moves between devices by JAX's collectives and lax.ppermute only.
A program may use at most 64 MiB of HBM per device.

```python
import jax
import jax.numpy as jnp
from jax import lax

D = 1024
HEADS = 8
HD = 128
USR_DEV = 1
CAND = 512
PREF = 512
ROWS_SHARD = 512
USERS = 8
ITEMS = 4096
N_USER = 8
N_HEAD = 2


def draw_block(key):
    key_full, key_perm, key_shuffle, key_offset = jax.random.split(key, 4)
    row_count = USR_DEV * CAND
    capacity = 2 * row_count // N_USER
    slot_count = N_USER * capacity
    shard_ids = jnp.arange(slot_count, dtype=jnp.int32) // capacity
    full_shard = jax.random.randint(key_full, (), 0, N_USER, dtype=jnp.int32)
    permuted = jax.random.permutation(key_perm, slot_count).astype(jnp.int32)
    priority = permuted + jnp.where(shard_ids == full_shard, slot_count, 0).astype(jnp.int32)
    ordering = jnp.argsort(-priority, stable=True)
    chosen = shard_ids[ordering[:row_count]]
    chosen = jax.random.permutation(key_shuffle, chosen)
    offsets = jax.random.randint(key_offset, (row_count,), 0, ROWS_SHARD, dtype=jnp.int32)
    return (chosen * ROWS_SHARD + offsets).astype(jnp.int32)


def draw_cand_ids(key, part):
    block_keys = jax.random.split(jax.random.fold_in(key, 71), N_USER)
    blocks = jax.vmap(draw_block)(block_keys)
    return blocks.reshape(USR_DEV * N_USER, CAND).astype(jnp.int32)


def set_ends(entries, own_key, low, largest):
    spot = [jax.random.randint(jax.random.fold_in(own_key, axis), (), 0, length) for axis, length in enumerate(entries.shape)]
    widest = entries.shape.index(max(entries.shape))
    neighbour = spot[:widest] + [(spot[widest] + 1) % entries.shape[widest]] + spot[widest + 1:]
    return entries.at[tuple(spot)].set(low).at[tuple(neighbour)].set(largest)


def level_of(stream_key, extent, shards, low, largest):
    def one(position, parts):
        heights = jax.random.uniform(jax.random.fold_in(jax.random.fold_in(stream_key, 6), position), (parts,), jnp.float32, low / len(shards), largest / len(shards))
        return jnp.repeat(jnp.exp(heights), extent[position] // parts).reshape((-1,) + (1,) * (len(extent) - position - 1))

    factor_of = one(*shards[0])
    for cut in shards[1:]:
        factor_of = factor_of * one(*cut)
    return factor_of


def bell_draw(rng, dims, deviation, limit, cuts=(), held_as=jnp.bfloat16):
    entries = jax.random.normal(rng, dims, jnp.float32) * deviation
    if len(cuts) > 0:
        entries = level_of(rng, dims, cuts, -0.22, 0.18) * entries
    return jnp.clip(entries, min=-limit, max=limit).astype(held_as)


def setup_inputs(seed: int = 0, part: int = 0) -> dict:
    keys = jax.random.split(jax.random.key(seed), 8)
    part_keys = jax.random.split(jax.random.fold_in(keys[7], part), 8)
    cand_ids = draw_cand_ids(jax.random.fold_in(jax.random.fold_in(keys[7], part), 71), part)
    prefix_len = set_ends(jax.random.randint(part_keys[1], (USERS,), 1, PREF + 1), jax.random.fold_in(part_keys[1], 1), 1, PREF).astype(jnp.int32)
    key_cache = bell_draw(part_keys[2], (USERS, PREF, D), 1.0, 6.0, ((0, 8), (2, 2)))
    value_cache = bell_draw(part_keys[3], (USERS, PREF, D), 1.0, 6.0, ((0, 8), (2, 2)))
    item_table = bell_draw(keys[4], (ITEMS, D), 1.0, 6.0, ((0, 8),))
    w_qkvu = bell_draw(keys[5], (D, HEADS, 4, HD), D ** -0.5, 0.1875, ((1, 2),))
    w_out = bell_draw(keys[6], (HEADS, HD, D), D ** -0.5, 0.1875, ((0, 2),))
    return {"cand_ids": cand_ids, "prefix_len": prefix_len, "key_cache": key_cache, "value_cache": value_cache, "item_table": item_table, "w_qkvu": w_qkvu, "w_out": w_out}


def reference(cand_ids, prefix_len, key_cache, value_cache, item_table, w_qkvu, w_out):
    score_scale = HD ** (-0.5)
    flat_weight = w_qkvu.reshape(D, HEADS * 4 * HD)
    group_width = HEADS // N_HEAD * HD
    w_groups = w_out.reshape(N_HEAD, group_width, D).astype(jnp.float32)

    def one_user(packed):
        item_ids, length, cached_keys, cached_values = packed
        embedded = item_table[item_ids.astype(jnp.int32)]
        projected = jnp.dot(embedded, flat_weight, preferred_element_type=jnp.float32)
        activated = jax.nn.silu(projected).astype(jnp.bfloat16).reshape(CAND, HEADS, 4, HD)
        queries = activated[:, :, 0].astype(jnp.float32)
        own_keys = activated[:, :, 1].astype(jnp.float32)
        own_values = activated[:, :, 2].astype(jnp.float32)
        gates = activated[:, :, 3].astype(jnp.float32)
        keys_all = cached_keys.reshape(PREF, HEADS, HD).astype(jnp.float32)
        values_all = cached_values.reshape(PREF, HEADS, HD).astype(jnp.float32)
        raw = jnp.einsum('chd,phd->hcp', queries, keys_all)
        denominator = (length + 1).astype(jnp.float32)
        in_prefix = jnp.arange(PREF, dtype=jnp.int32) < length
        weights = jnp.where(in_prefix[None, None, :], jax.nn.silu(raw * score_scale), 0.0) / denominator
        weights = weights.astype(jnp.bfloat16).astype(jnp.float32)
        attended = jnp.einsum('hcp,phd->chd', weights, values_all)
        own_weight = jax.nn.silu(lax.optimization_barrier(jnp.sum(queries * own_keys, axis=-1)) * score_scale) / denominator
        attended = attended + own_weight[:, :, None] * own_values
        mean_square = lax.optimization_barrier(jnp.mean(attended * attended, axis=-1, keepdims=True))
        gated = (attended * lax.rsqrt(mean_square + 1e-06) * gates).astype(jnp.bfloat16)
        group_rows = gated.reshape(CAND, N_HEAD, group_width).astype(jnp.float32)
        partial_value = jnp.einsum('cgk,gkd->gcd', group_rows, w_groups).astype(jnp.bfloat16)
        summed = lax.optimization_barrier(jnp.sum(partial_value.astype(jnp.float32), axis=0))
        inner = lax.optimization_barrier(jnp.sum(summed * embedded.astype(jnp.float32), axis=-1)) * D ** (-0.5)
        return inner * lax.rsqrt(lax.optimization_barrier(jnp.mean(summed * summed, axis=-1)) + 1e-06)
    return lax.map(one_user, (cand_ids, prefix_len, key_cache, value_cache))
```

```python
import functools

import jax
import jax.numpy as jnp
from jax import lax
from jax.experimental import pallas as pl
from jax.experimental.pallas import tpu as pltpu
from jax.sharding import PartitionSpec as P

AXES = ("grp", "user", "head")


def silu_f32(value):
    half = 0.5 * value
    return half + half * jnp.tanh(half)


def select_kernel(base_ref, ids_ref, *refs, pieces, groups, has_prev):
    piece_refs = refs[:pieces]
    prev_refs = refs[pieces : pieces + groups] if has_prev else None
    out_refs = refs[len(refs) - groups - 1 : len(refs) - 1]
    hot_ref = refs[-1]
    rows = piece_refs[0].shape[0]
    count = ids_ref.shape[1]
    step = min(count, 128)
    for j in range(groups):
        for i in range(pieces):
            for start in range(0, count, step):
                local = ids_ref[j, start : start + step, :] - base_ref[i]
                lane = lax.broadcasted_iota(jnp.int32, (step, rows), 1)
                hot_ref[start : start + step, i * rows : (i + 1) * rows] = jnp.where(
                    lane == local, 1.0, 0.0
                ).astype(jnp.bfloat16)
        total = None
        for i in range(pieces):
            part = jnp.dot(
                hot_ref[:, i * rows : (i + 1) * rows],
                piece_refs[i][...],
                preferred_element_type=jnp.float32,
            )
            total = part if total is None else total + part
        if has_prev:
            total = total + prev_refs[j][...].astype(jnp.float32)
        out_refs[j][...] = total.astype(jnp.bfloat16)


def select_rows(bases, ids, pieces, prev=None):
    groups, count = ids.shape[0], ids.shape[1]
    rows, feats = pieces[0].shape
    vmem = pl.BlockSpec(memory_space=pltpu.VMEM)
    extra = [] if prev is None else list(prev)
    return pl.pallas_call(
        functools.partial(
            select_kernel, pieces=len(pieces), groups=groups, has_prev=prev is not None
        ),
        out_shape=[jax.ShapeDtypeStruct((count, feats), jnp.bfloat16)] * groups,
        in_specs=[pl.BlockSpec(memory_space=pltpu.SMEM)] + [vmem] * (1 + len(pieces) + len(extra)),
        out_specs=[vmem] * groups,
        scratch_shapes=[pltpu.VMEM((count, rows * len(pieces)), jnp.bfloat16)],
        cost_estimate=pl.CostEstimate(
            flops=2 * groups * count * rows * len(pieces) * feats,
            bytes_accessed=2 * rows * len(pieces) * feats,
            transcendentals=0,
        ),
        name="select_rows",
    )(bases, ids, *pieces, *extra)


def attend_kernel(int_ref, float_ref, *refs, parts, scale):
    part_refs = refs[:parts]
    w_ref, k_ref, v_ref, out_ref = refs[parts:]
    feats = part_refs[0].shape[1]
    rows = out_ref.shape[0]
    size = k_ref.shape[1]
    length = int_ref[parts]
    inverse = float_ref[0]
    position = lax.broadcasted_iota(jnp.int32, v_ref.shape, 0)
    values = jnp.where(position < length, v_ref[...].astype(jnp.float32), 0.0).astype(jnp.bfloat16)
    step = min(rows, 256)
    for start in range(0, rows, step):
        projected = None
        for i in range(parts):
            w_rows = w_ref[pl.ds(pl.multiple_of(int_ref[i] * feats, feats), feats), :]
            piece = jnp.dot(
                part_refs[i][start : start + step, :], w_rows, preferred_element_type=jnp.float32
            )
            projected = piece if projected is None else projected + piece
        activated = silu_f32(projected).astype(jnp.bfloat16)
        queries = activated[:, :size]
        own_keys = activated[:, size : 2 * size].astype(jnp.float32)
        own_values = activated[:, 2 * size : 3 * size].astype(jnp.float32)
        gates = activated[:, 3 * size :].astype(jnp.float32)
        raw = lax.dot_general(
            queries, k_ref[...], (((1,), (1,)), ((), ())), preferred_element_type=jnp.float32
        )
        weights = (silu_f32(raw * scale) * inverse).astype(jnp.bfloat16)
        attended = jnp.dot(weights, values, preferred_element_type=jnp.float32)
        own_dot = jnp.sum(queries.astype(jnp.float32) * own_keys, axis=-1, keepdims=True)
        attended = attended + (silu_f32(own_dot * scale) * inverse) * own_values
        mean_square = jnp.mean(attended * attended, axis=-1, keepdims=True)
        out_ref[start : start + step, :] = (
            attended * lax.rsqrt(mean_square + 1e-06) * gates
        ).astype(jnp.bfloat16)


def attend(ints, floats, parts, w_flat, keys, values, heads, size):
    rows, feats = parts[0].shape
    width = w_flat.shape[0]
    prefix = keys.shape[0]
    smem = pl.BlockSpec(memory_space=pltpu.SMEM)
    return pl.pallas_call(
        functools.partial(attend_kernel, parts=len(parts), scale=size ** (-0.5)),
        grid=(heads,),
        out_shape=jax.ShapeDtypeStruct((rows, heads * size), jnp.bfloat16),
        in_specs=[smem, smem]
        + [pl.BlockSpec((rows, feats), lambda j: (0, 0))] * len(parts)
        + [
            pl.BlockSpec((width, 4 * size), lambda j: (0, j)),
            pl.BlockSpec((prefix, size), lambda j: (0, j)),
            pl.BlockSpec((prefix, size), lambda j: (0, j)),
        ],
        out_specs=pl.BlockSpec((rows, size), lambda j: (0, j)),
        cost_estimate=pl.CostEstimate(
            flops=2 * rows * heads * size * (4 * width + 2 * prefix),
            bytes_accessed=2 * (w_flat.size + keys.size + values.size + 2 * rows * width),
            transcendentals=rows * heads * (4 * size + prefix),
        ),
        name="attend",
    )(ints, floats, *parts, w_flat, keys, values)


def lane_sum_row(product):
    rows, width = product.shape
    folded = product[:, :128]
    for start in range(128, width, 128):
        folded = folded + product[:, start : start + 128]
    return jnp.sum(folded.T, axis=0, keepdims=True)


def score_kernel(int_ref, *refs, parts, groups, width):
    gated_refs = refs[:groups]
    w_refs = refs[groups : 2 * groups]
    part_refs = refs[2 * groups : 2 * groups + parts]
    out_ref, sum_ref = refs[2 * groups + parts :]
    feats = part_refs[0].shape[1]
    summed = None
    for i in range(groups):
        partial = jnp.dot(
            gated_refs[i][...], w_refs[i][...], preferred_element_type=jnp.float32
        ).astype(jnp.bfloat16).astype(jnp.float32)
        summed = partial if summed is None else summed + partial
    square = lane_sum_row(summed * summed)
    for i in range(width // feats):
        sum_ref[i] = summed[:, i * feats : (i + 1) * feats]
    product = None
    for i in range(parts):
        term = sum_ref[int_ref[i]] * part_refs[i][...].astype(jnp.float32)
        product = term if product is None else product + term
    inner = lane_sum_row(product)
    out_ref[...] = inner * width ** (-0.5) * lax.rsqrt(square * (1.0 / width) + 1e-06)


def score_rows(ints, row_block, gated, w_out, parts, rows):
    groups = len(gated)
    feats = parts[0].shape[1]
    width = w_out[0].shape[1]
    depth = w_out[0].shape[0]
    block = lambda c: pl.BlockSpec((rows, c), lambda i, ints: (ints[len(parts)], 0))
    whole = lambda r, c: pl.BlockSpec((r, c), lambda i, ints: (0, 0))
    return pl.pallas_call(
        functools.partial(score_kernel, parts=len(parts), groups=groups, width=width),
        grid_spec=pltpu.PrefetchScalarGridSpec(
            num_scalar_prefetch=1,
            grid=(1,),
            in_specs=[block(depth)]
            + [whole(rows, depth)] * (groups - 1)
            + [whole(depth, width)] * groups
            + [block(feats)] * len(parts),
            out_specs=whole(1, rows),
            scratch_shapes=[pltpu.VMEM((width // feats, rows, feats), jnp.float32)],
        ),
        out_shape=jax.ShapeDtypeStruct((1, rows), jnp.float32),
        cost_estimate=pl.CostEstimate(
            flops=2 * rows * groups * depth * width,
            bytes_accessed=2 * groups * depth * width,
            transcendentals=rows,
        ),
        name="score_rows",
    )(ints, *gated, *w_out, *parts)


def body(cand_ids, prefix_len, key_cache, value_cache, item_table, w_qkvu, w_out):
    grp_size, user_size, head_size = (lax.axis_size(name) for name in AXES)
    grp, user, head = (lax.axis_index(name) for name in AXES)
    cand_count = cand_ids.shape[0] * cand_ids.shape[1]
    rows_shard, width = item_table.shape
    heads_here, size = w_qkvu.shape[1], w_qkvu.shape[3]
    prefix = key_cache.shape[1]
    columns = grp_size * head_size
    feats = width // columns

    def device(g, u, h):
        return (g * user_size + u) * head_size + h

    def move(value, target):
        pairs = [
            (device(g, u, h), device(*target(g, u, h)))
            for g in range(grp_size)
            for u in range(user_size)
            for h in range(head_size)
        ]
        return lax.ppermute(value, AXES, pairs)

    column = grp * head_size + head
    own = lax.dynamic_slice_in_dim(item_table, column * feats, feats, 1)
    ids = [cand_ids.reshape(-1)]
    for dg in range(1, grp_size):
        ids.append(move(ids[0], lambda g, u, h, dg=dg: ((g - dg) % grp_size, u, h)))
    ids = jnp.stack(ids).reshape(grp_size, cand_count, 1)
    pieces, masks = [own], [0]
    distance = user_size // 2
    while distance >= 1:
        pieces += [move(p, lambda g, u, h: (g, u ^ distance, h)) for p in pieces]
        masks += [m | distance for m in masks]
        distance //= 2
    bases = [(user ^ m) * rows_shard for m in masks]
    late = [i for i, m in enumerate(masks) if m | 1 == user_size - 1]
    early = [i for i in range(len(masks)) if i not in late]
    take = lambda values, where: [values[i] for i in where]
    chosen = None
    if early:
        chosen = select_rows(jnp.stack(take(bases, early)), ids, take(pieces, early))
    chosen = select_rows(jnp.stack(take(bases, late)), ids, take(pieces, late), chosen)

    parts, order = [chosen[0]], [column]
    for dg in range(grp_size):
        for dh in range(head_size):
            if dg == 0 and dh == 0:
                continue
            parts.append(
                move(
                    chosen[dg],
                    lambda g, u, h: ((g + dg) % grp_size, u, (h + dh) % head_size),
                )
            )
            order.append(
                ((grp - dg) % grp_size) * head_size + (head - dh) % head_size
            )

    ints = jnp.stack(order + [prefix_len[0]]).astype(jnp.int32)
    inverse = 1.0 / (prefix_len + 1).astype(jnp.float32)
    gated = attend(
        ints,
        inverse,
        parts,
        w_qkvu.reshape(width, heads_here * 4 * size),
        key_cache.reshape(prefix, heads_here * size),
        value_cache.reshape(prefix, heads_here * size),
        heads_here,
        size,
    )

    rows = cand_count // head_size
    w_here = w_out.reshape(heads_here * size, width)
    gated_parts, w_parts = [gated], [w_here]
    for dh in range(1, head_size):
        target = lambda g, u, h: (g, u, (h + dh) % head_size)
        block = lax.dynamic_slice_in_dim(gated, ((head + dh) % head_size) * rows, rows, 0)
        gated_parts.append(move(block, target))
        w_parts.append(move(w_here, target))
    score_ints = jnp.stack(order + [head]).astype(jnp.int32)
    mine = score_rows(score_ints, head, gated_parts, w_parts, parts, rows)
    blocks = [mine]
    for dh in range(1, head_size):
        blocks.append(move(mine, lambda g, u, h: (g, u, (h - dh) % head_size)))
    ordered = []
    for b in range(head_size):
        value = blocks[0]
        for dh in range(1, head_size):
            value = jnp.where((head + dh) % head_size == b, blocks[dh], value)
        ordered.append(value)
    return jnp.concatenate(ordered, axis=1).reshape(cand_ids.shape)


def solution(mesh):
    in_specs = (
        P(("grp", "user"), None),
        P(("grp", "user")),
        P(("grp", "user"), None, "head"),
        P(("grp", "user"), None, "head"),
        P("user", None),
        P(None, "head", None, None),
        P("head", None, None),
    )
    out_specs = P(("grp", "user"), None)
    return jax.shard_map(body, mesh=mesh, in_specs=in_specs, out_specs=out_specs, check_vma=False)
```
